32 devices in a mesh: row: 2 (over x), col: 16 (over z, y, core).
Axes of the slice: x: 2, y: 2, z: 4, core: 2. Of those that a mesh axis runs over, the one named last changes fastest.
Arguments:
- tokens: bfloat16 [512, 4608], P('col', 'row'), may hold values from -6 to 6
- pre_gain: float32 [2, 4608], P(None, 'row'), may hold values from -0.6 to 0.6
- post_gain: float32 [2, 4608], P(None, 'row'), may hold values from -0.6 to 0.6
- gate_weight: bfloat16 [2, 4608, 36864], P(None, ('row', 'col')), may hold values from -0.09375 to 0.09375
- up_weight: bfloat16 [2, 4608, 36864], P(None, ('row', 'col')), may hold values from -0.09375 to 0.09375
- down_weight: bfloat16 [2, 36864, 4608], P(None, ('row', 'col')), may hold values from -0.13541667 to 0.13541667
Outputs:
- stream: bfloat16 [512, 4608], P('col', 'row')
The draws below stay inside these ranges and needn't reach their ends.
All inputs are finite; a program needn't handle non-finite values.
Results may differ from the reference program's by a relative error of at most 0.019.
Values may be sent and summed in bfloat16 or wider, within the bound.
A program may use at most 256 MiB of HBM per device.

```python
import math
import jax
import jax.numpy as jnp
from jax import lax

D = 4608
FF = 36864
LAYERS = 2
TOKENS = 512


def draw_down_weight(key, part):
    key_main = jax.random.fold_in(key, 11)
    key_rough = jax.random.fold_in(key, 12)
    entries = jax.random.truncated_normal(key_main, -6.0, 6.0, (LAYERS, FF, D), jnp.float32)
    low_end = 0.5
    high_end = 2.0
    ramp = jnp.linspace(math.log(low_end), math.log(high_end), D, dtype=jnp.float32)
    rough = jax.random.uniform(key_rough, (LAYERS, 1, D), jnp.float32, math.log(0.7), math.log(1.4))
    scales = jnp.exp(ramp[None, None, :] + rough)
    return (entries * scales * FF ** (-0.5)).astype(jnp.bfloat16)


def block_levels(own_key, shape, shards, least, top_value):
    loudness = 1.0
    for axis_at, blocks in shards:
        draws = jax.random.uniform(jax.random.fold_in(jax.random.fold_in(own_key, 6), axis_at), (blocks,), jnp.float32, least / len(shards), top_value / len(shards))
        loudness = loudness * jnp.repeat(jnp.exp(draws), shape[axis_at] // blocks).reshape((-1,) + (1,) * (len(shape) - 1 - axis_at))
    return loudness


def bell_draw(stream_key, extent, scale, most, pieces=(), held_as=jnp.bfloat16):
    drawn = jax.random.normal(stream_key, extent, jnp.float32) * scale
    if len(pieces) > 0:
        drawn = block_levels(stream_key, extent, pieces, -0.22, 0.18) * drawn
    return jnp.clip(drawn, min=-most, max=most).astype(held_as)


def setup_inputs(seed: int = 0) -> dict:
    seeds = jax.random.split(jax.random.key(seed), 7)
    return {
        "tokens": bell_draw(seeds[0], (TOKENS, D), 1.0, 6.0, ((0, 16), (1, 2))),
        "pre_gain": jnp.clip(jax.random.uniform(seeds[1], (LAYERS, D), jnp.float32, -0.6, 0.6) * block_levels(seeds[1], (LAYERS, D), ((1, 2),), -0.4, 0.0), -0.6, 0.6),
        "post_gain": jnp.clip(jax.random.uniform(seeds[2], (LAYERS, D), jnp.float32, -0.6, 0.6) * block_levels(seeds[2], (LAYERS, D), ((1, 2),), -0.4, 0.0), -0.6, 0.6),
        "gate_weight": bell_draw(seeds[3], (LAYERS, D, FF), D ** -0.5, 0.09375, ((1, 32),)),
        "up_weight": bell_draw(seeds[4], (LAYERS, D, FF), D ** -0.5, 0.09375, ((1, 32),)),
        "down_weight": draw_down_weight(jax.random.fold_in(seeds[6], 71), 0),
    }


norm_eps = 1e-06

def reference(tokens, pre_gain, post_gain, gate_weight, up_weight, down_weight):
    current = tokens
    for layer_index in range(LAYERS):
        values = current.astype(jnp.float32)
        mean_sq = lax.optimization_barrier(jnp.mean(values * values, axis=1, keepdims=True))
        normed = (values * lax.rsqrt(mean_sq + norm_eps) * (1.0 + pre_gain[layer_index])[None, :]).astype(jnp.bfloat16)
        gate = jnp.dot(normed, gate_weight[layer_index], preferred_element_type=jnp.float32)
        up_proj = jnp.dot(normed, up_weight[layer_index], preferred_element_type=jnp.float32)
        hidden = (jax.nn.gelu(gate, approximate=True) * up_proj).astype(jnp.bfloat16)
        branch = jnp.dot(hidden, down_weight[layer_index], preferred_element_type=jnp.float32)
        branch_sq = lax.optimization_barrier(jnp.mean(branch * branch, axis=1, keepdims=True))
        post = branch * lax.rsqrt(branch_sq + norm_eps) * (1.0 + post_gain[layer_index])[None, :]
        current = (values + post).astype(jnp.bfloat16)
    return current
```

```python
import jax
import jax.numpy as jnp
from jax import lax
from jax.sharding import PartitionSpec as P

norm_eps = 1e-06
AXES = ("row", "col")


def activate(gate, up_proj):
    return (jax.nn.gelu(gate, approximate=True) * up_proj).astype(jnp.bfloat16)


def make_on_device(row_count, col_count):
    planes = 4 if col_count % 4 == 0 else 1
    inner = col_count // planes
    members = row_count * inner

    def swap(array, row_bits, plane_bits, seat_bits):
        pairs = []
        for row in range(row_count):
            for plane in range(planes):
                for seat in range(inner):
                    source = row * col_count + plane * inner + seat
                    target = (
                        (row ^ row_bits) * col_count
                        + (plane ^ plane_bits) * inner
                        + (seat ^ seat_bits)
                    )
                    pairs.append((source, target))
        return lax.ppermute(array, AXES, pairs)

    def sum_over_rows(array):
        total = array
        for bits in range(1, row_count):
            total = total + swap(array, bits, 0, 0)
        return total

    def on_device(tokens, pre_gain, post_gain, gate_weight, up_weight, down_weight):
        layer_count = gate_weight.shape[0]
        own_tokens, own_width = tokens.shape
        model_width = own_width * row_count
        stored_rows = gate_weight.shape[1]
        block_width = gate_weight.shape[2] // (row_count * col_count)
        plane_width = own_width // planes
        row = lax.axis_index("row")
        col = lax.axis_index("col")
        plane = col // inner
        seat = col % inner
        member = row * inner + seat

        def weight_chunk(layer_index, plane_bits):
            chunk_plane = plane ^ plane_bits
            held = jnp.zeros((members, stored_rows, 2 * block_width), jnp.bfloat16)
            for bits in range(members):
                row_bits, seat_bits = bits // inner, bits % inner
                start = (
                    (row ^ row_bits) * col_count + chunk_plane * inner + (seat ^ seat_bits)
                ) * block_width
                gate_part, up_part = (
                    lax.dynamic_slice(
                        weight, (layer_index, 0, start), (1, stored_rows, block_width)
                    )
                    for weight in (gate_weight, up_weight)
                )
                block = jnp.concatenate((gate_part, up_part), axis=2)
                if bits:
                    block = swap(block, row_bits, 0, seat_bits)
                held = lax.dynamic_update_slice(held, block, (member ^ bits, 0, 0))
            return held.reshape(members * stored_rows, 2 * block_width)

        def gather_plane(normed):
            parts = normed.reshape(own_tokens, planes, plane_width).transpose(1, 0, 2)
            held = jnp.zeros((planes, own_tokens, plane_width), jnp.bfloat16)
            for bits in range(planes):
                part = lax.dynamic_slice(
                    parts, (plane ^ bits, 0, 0), (1, own_tokens, plane_width)
                )
                if bits:
                    part = swap(part, 0, bits, 0)
                held = lax.dynamic_update_slice(held, part, (plane ^ bits, 0, 0))
            pieces = [held]
            for bits in range(1, row_count):
                pieces.append(swap(held, bits, 0, 0))
            rows = jnp.zeros((row_count,) + held.shape, jnp.bfloat16)
            for bits in range(row_count):
                rows = lax.dynamic_update_slice(rows, pieces[bits][None], (row ^ bits, 0, 0, 0))
            whole = rows.transpose(1, 2, 0, 3).reshape(
                planes, 1, own_tokens, row_count * plane_width
            )
            bit = inner // 2
            order = [0]
            blocks = whole
            while bit:
                blocks = jnp.concatenate((blocks, swap(blocks, 0, 0, bit)), axis=1)
                order = order + [seat_bits ^ bit for seat_bits in order]
                bit //= 2
            return blocks.reshape(planes * inner * own_tokens, row_count * plane_width), order

        def scatter_branch(branch):
            bit = 1
            halved_rows = False
            while bit < inner or not halved_rows:
                if bit < inner:
                    half = branch.shape[1] // 2
                    away = branch[:, half:].astype(jnp.bfloat16)
                    branch = branch[:, :half] + swap(away, 0, 0, bit).astype(jnp.float32)
                    bit *= 2
                if not halved_rows:
                    split = [
                        branch[..., i * own_width : (i + 1) * own_width]
                        for i in range(row_count)
                    ]

                    def part_of(wanted):
                        chosen = split[0]
                        for i in range(1, row_count):
                            chosen = jnp.where(wanted == i, split[i], chosen)
                        return chosen

                    total = part_of(row)
                    for bits in range(1, row_count):
                        away = part_of(row ^ bits).astype(jnp.bfloat16)
                        total = total + swap(away, bits, 0, 0).astype(jnp.float32)
                    branch = total
                    halved_rows = True
            branch = branch.reshape(planes, own_tokens, own_width)
            total = lax.dynamic_slice(branch, (plane, 0, 0), (1, own_tokens, own_width))
            for bits in range(1, planes):
                away = lax.dynamic_slice(
                    branch, (plane ^ bits, 0, 0), (1, own_tokens, own_width)
                ).astype(jnp.bfloat16)
                total = total + swap(away, 0, bits, 0).astype(jnp.float32)
            return total[0]

        current = tokens
        for layer_index in range(layer_count):
            values = current.astype(jnp.float32)
            squares = sum_over_rows(jnp.sum(values * values, axis=1, keepdims=True))
            scale_pre = lax.rsqrt(squares / model_width + norm_eps)
            normed = (values * scale_pre * (1.0 + pre_gain[layer_index])[None, :]).astype(
                jnp.bfloat16
            )
            gathered, order = gather_plane(normed)
            arrived = []
            for bits in reversed(range(planes)):
                chunk = weight_chunk(layer_index, bits)
                part = jnp.dot(gathered, chunk, preferred_element_type=jnp.float32)
                if bits:
                    part = swap(part.astype(jnp.bfloat16), 0, bits, 0)
                arrived.append(part)
            summed = arrived[-1]
            for part in arrived[:-1]:
                summed = summed + part.astype(jnp.float32)
            hidden = activate(summed[:, :block_width], summed[:, block_width:])
            branch = jnp.dot(hidden, down_weight[layer_index], preferred_element_type=jnp.float32)
            branch = branch.reshape(planes, inner, own_tokens, model_width)
            branch = scatter_branch(branch)
            branch_squares = sum_over_rows(jnp.sum(branch * branch, axis=1, keepdims=True))
            scale_post = lax.rsqrt(branch_squares / model_width + norm_eps)
            post = branch * scale_post * (1.0 + post_gain[layer_index])[None, :]
            current = (values + post).astype(jnp.bfloat16)
        return current

    return on_device


def solution(mesh):
    in_specs = (
        P("col", "row"),
        P(None, "row"),
        P(None, "row"),
        P(None, ("row", "col"), None),
        P(None, ("row", "col"), None),
        P(None, ("row", "col"), None),
    )
    out_specs = P("col", "row")
    on_device = make_on_device(mesh.shape["row"], mesh.shape["col"])
    return jax.shard_map(
        on_device, mesh=mesh, in_specs=in_specs, out_specs=out_specs, check_vma=False
    )
```
